256 devices in a mesh: seq: 32 (over z, x_hi, core), head: 4 (over y), batch: 2 (over x_lo).
Axes of the slice: x: 4 (x_hi: 2, x_lo: 2; x = x_hi * 2 + x_lo), y: 4, z: 8, core: 2. Of those that a mesh axis runs over, the one named last changes fastest.
Arguments:
- queries: bfloat16 [16384, 4096], P(('batch', 'seq', 'head')), parts along dimension 0, may hold values from -6 to 6
- keys: bfloat16 [16384, 512], P(('batch', 'seq', 'head')), parts along dimension 0, may hold values from -6 to 6
- values: bfloat16 [16384, 512], P(('batch', 'seq', 'head')), parts along dimension 0, may hold values from -6 to 6
- page_of_block: int32 [32], P('batch'), parts along dimension 0, may hold values from 0 to 8, never falling along the last dimension, each value on 1 to 4 neighbouring positions
- links: int32 [32, 16], P('batch'), parts along dimension 0, may hold values 0 or 1
Outputs:
- attended: bfloat16 [16384, 4096], P(('batch', 'seq', 'head')), parts along dimension 0
The draws below stay inside these ranges and needn't reach their ends.
There are 2 independent parts, one for each index of `batch`. The reference program is written for one: setup_inputs(seed, part) draws one part's arguments, and reference() takes and returns one part's arrays. A program takes and returns all parts, laid end to end along the dimension named above; each array names one. Nothing has to cross between parts.
Inputs may be any that keep to these rules, and one draw needn't show every extreme that they name: `page_of_block`: page numbers never fall from one block to the next.
All inputs are finite; a program needn't handle non-finite values.
Results may differ from the reference program's by a relative error of at most 0.0065.
Values may be sent and summed in bfloat16 or wider, within the bound.
A program may use at most 64 MiB of HBM per device.

```python
import math
import jax
import jax.numpy as jnp
import numpy as np
from jax import lax

QUERY_HEAD_COUNT = 32
KEY_VALUE_HEADS = 4
HEAD_SIZE = 128
BLK = 512
SEQUENCE_TOKENS = 8192
NB = 16


def draw_queries(key, part):
    starting_point = jnp.clip(jax.random.normal(jax.random.fold_in(key, 11), (SEQUENCE_TOKENS, QUERY_HEAD_COUNT, HEAD_SIZE), jnp.float32), -6.0, 6.0)
    return starting_point.reshape(SEQUENCE_TOKENS, QUERY_HEAD_COUNT * HEAD_SIZE).astype(jnp.bfloat16)


def draw_keys(key, part):
    starting_point = jnp.clip(jax.random.normal(jax.random.fold_in(key, 23), (SEQUENCE_TOKENS, KEY_VALUE_HEADS, HEAD_SIZE), jnp.float32), -6.0, 6.0)
    return starting_point.reshape(SEQUENCE_TOKENS, KEY_VALUE_HEADS * HEAD_SIZE).astype(jnp.bfloat16)


def plant(result, key, least, largest):
    longest = result.shape.index(max(result.shape))
    spots = []
    for shift in (0, 1):
        where = [jax.random.randint(jax.random.fold_in(key, axis), (), 0, length) for axis, length in enumerate(result.shape)]
        where[longest] = (where[longest] + shift) % result.shape[longest]
        spots.append(tuple(where))
    return result.at[spots[0]].set(least).at[spots[1]].set(largest)


def levels(rng, dims, cuts, low, top_value):
    factor_of, own = 1.0, jax.random.fold_in(rng, 6)
    for dim, parts in cuts:
        heights = jnp.exp(jax.random.uniform(jax.random.fold_in(own, dim), (parts,), jnp.float32, low / len(cuts), top_value / len(cuts)))
        factor_of = factor_of * jnp.repeat(heights, dims[dim] // parts).reshape([-1 if axis == dim else 1 for axis in range(len(dims))])
    return factor_of


def profile(amount, total, reach, lean):
    weights = [(1 << 20) // math.isqrt(grade ** lean) + 1 for grade in range(2, amount + 1)]
    surplus, counts = total - reach - (amount - 1), [1] * (amount - 1)
    while surplus > 0:
        free = [i for i in range(amount - 1) if counts[i] < reach]
        mass, left = sum([weights[i] for i in free]), surplus
        for i in free:
            addition = min(reach - counts[i], max(1, left * weights[i] // mass), surplus)
            counts[i] = counts[i] + addition
            surplus = surplus - addition
    return np.array([reach] + counts)


def uneven(stream_key, count, total, bound, lean):
    if count == 2:
        one = jax.random.randint(stream_key, (), max(1, total - bound), min(bound, total - 1) + 1)
        return jnp.stack([one, total - one])
    tallies = jnp.asarray(profile(count, total, bound, lean), jnp.int32)
    pairs = (count - 1) // 2
    giver, sink = tallies[1:1 + 2 * pairs:2], tallies[2:2 + 2 * pairs:2]
    room = jnp.minimum(giver - 1, bound - sink)
    shifted = jax.random.randint(jax.random.fold_in(stream_key, 1), (pairs,), 0, 1 << 20) % (room + 1)
    tallies = tallies.at[1:1 + 2 * pairs:2].set(giver - shifted).at[2:2 + 2 * pairs:2].set(sink + shifted)
    return tallies[jax.random.permutation(jax.random.fold_in(stream_key, 2), count)]


def normal_values(rng, dims, scale, reach, cuts=(), kind=jnp.bfloat16):
    drawn = scale * jax.random.normal(rng, dims, jnp.float32)
    if cuts:
        drawn = drawn * levels(rng, dims, cuts, -0.22, 0.18)
    return jnp.clip(drawn, -reach, reach).astype(kind)


def setup_inputs(seed: int = 0, part: int = 0) -> dict:
    streams_of = jax.random.split(jax.random.key(seed), 6)
    part_splits = jax.random.split(jax.random.fold_in(streams_of[5], part), 6)
    queries = draw_queries(jax.random.fold_in(jax.random.fold_in(streams_of[5], part), 71), part)
    keys = draw_keys(jax.random.fold_in(jax.random.fold_in(streams_of[5], part), 71), part)
    values = normal_values(part_splits[2], (SEQUENCE_TOKENS, KEY_VALUE_HEADS * HEAD_SIZE), 1.0, 6.0, ((0, 128),))
    page_of_block = jnp.searchsorted(jnp.cumsum(uneven(part_splits[3], NB // 2 + 1, NB, min(4, NB - NB // 2), 2)), jnp.arange(NB), side="right").astype(jnp.int32)
    links = plant((jax.random.randint(part_splits[4], (NB, NB), 0, 4) < 1).astype(jnp.int32), jax.random.fold_in(part_splits[4], 1), 0, 1)
    return dict(queries=queries, keys=keys, values=values, page_of_block=page_of_block, links=links)


def reference(queries, keys, values, page_of_block, links):
    position = jnp.arange(SEQUENCE_TOKENS, dtype=jnp.int32)
    block_of = position // BLK
    page_ids = page_of_block[block_of]
    same_page = page_ids[:, None] == page_ids[None, :]
    causal = position[None, :] <= position[:, None]
    linked = jnp.repeat(jnp.repeat(links == 1, BLK, axis=0), BLK, axis=1)
    allowed = jnp.where(same_page, causal, linked)
    group_width = QUERY_HEAD_COUNT // KEY_VALUE_HEADS
    query_heads = queries.reshape(SEQUENCE_TOKENS, QUERY_HEAD_COUNT, HEAD_SIZE).transpose(1, 0, 2)
    heads_of_keys = jnp.repeat(keys.reshape(SEQUENCE_TOKENS, KEY_VALUE_HEADS, HEAD_SIZE).transpose(1, 0, 2), group_width, axis=0)
    heads_of_values = jnp.repeat(values.reshape(SEQUENCE_TOKENS, KEY_VALUE_HEADS, HEAD_SIZE).transpose(1, 0, 2), group_width, axis=0)

    def one_head(triple):
        query_head, key_head, value_head = triple
        scores = jnp.dot(query_head, key_head.T, preferred_element_type=jnp.float32) * (HEAD_SIZE ** -0.5)
        scores = jnp.where(allowed, scores, -1e30)
        maximum = jnp.max(scores, axis=1, keepdims=True)
        weights = jnp.where(allowed, jnp.exp(scores - maximum), 0.0)
        totals = jnp.sum(weights, axis=1, keepdims=True)
        mixture = jnp.dot(weights.astype(jnp.bfloat16), value_head, preferred_element_type=jnp.float32)
        return mixture / totals

    attended = lax.map(one_head, (query_heads, heads_of_keys, heads_of_values))
    return attended.transpose(1, 0, 2).reshape(SEQUENCE_TOKENS, QUERY_HEAD_COUNT * HEAD_SIZE).astype(jnp.bfloat16)
```

```python
import jax
import jax.numpy as jnp
from jax import lax
from jax.experimental import pallas as pl
from jax.experimental.pallas import tpu as pltpu
from jax.sharding import PartitionSpec as P

HEAD_SIZE = 128
BLK = 512
BLOCKS = 16
HEADS = 8
SEQ = 32
TOKENS = 64
ROWS = 256
WIDE = HEADS * HEAD_SIZE
UNIT = 2
UNITS = HEADS // UNIT
M = UNIT * ROWS
SCALE = HEAD_SIZE ** (-0.5) * 1.4426950408889634
NEG = -1e30
NT = (((1,), (1,)), ((), ()))
F32, BF16 = jnp.float32, jnp.bfloat16


def kernel(
    page_ref, link_ref, q_ref, k_ref, v_ref, out_ref,
    kv, qb, ost, m_s, acc_s, s_s, sh_s, al_s,
    a2a_send, a2a_recv, q_send, q_recv, ring_send, ring_recv, sib_send, sib_recv, out_send, out_recv, loc,
):
    seq, head = lax.axis_index("seq"), lax.axis_index("head")
    z, xh, core = seq // 4, (seq // 2) % 2, seq % 2
    own = seq // 2
    sibling = seq + 1 - 2 * core
    partner = seq + 2 - 4 * xh
    up, down = (seq + 4) % SEQ, (seq + SEQ - 4) % SEQ
    peers = [(head + d) % 4 for d in range(4)]
    half = pl.ds(pl.multiple_of(core * ROWS, ROWS), ROWS)

    def remote(src, dst, send, recv, **where):
        return pltpu.make_async_remote_copy(
            src_ref=src, dst_ref=dst, send_sem=send, recv_sem=recv,
            device_id=where, device_id_type=pl.DeviceIdType.MESH,
        )

    def kv_piece(xo, d, kind):
        src = (k_ref, v_ref)[kind].at[:, pl.ds(pl.multiple_of(peers[d] * HEAD_SIZE, HEAD_SIZE), HEAD_SIZE)]
        dst = kv.at[own, kind, pl.ds(pl.multiple_of(core * ROWS + head * TOKENS, TOKENS), TOKENS), :]
        if xo == 0 and d == 0:
            return pltpu.make_async_copy(src, dst, loc.at[kind])
        where = {"head": peers[d]} if xo == 0 else {"seq": partner, "head": peers[d]}
        return remote(src, dst, a2a_send.at[xo, d, kind], a2a_recv.at[xo, d, kind], **where)

    def q_piece(d, part):
        src = q_ref.at[:, pl.ds(pl.multiple_of(peers[d] * WIDE + part * (WIDE // 2), WIDE // 2), WIDE // 2)]
        dst = qb.at[pl.ds(pl.multiple_of(head * TOKENS, TOKENS), TOKENS), pl.ds(part * (WIDE // 2), WIDE // 2)]
        if d == 0:
            return pltpu.make_async_copy(src, dst, loc.at[2 + part])
        return remote(src, dst, q_send.at[d, part], q_recv.at[d, part], head=peers[d])

    def ring(block, way, step, kind):
        ref = kv.at[block, kind, half, :]
        to = up + way * (down - up)
        return remote(ref, ref, ring_send.at[way, step, kind], ring_recv.at[way, step, kind], seq=to)

    def share(pos, block, kind):
        ref = kv.at[block, kind, half, :]
        return remote(ref, ref, sib_send.at[pos, kind], sib_recv.at[pos, kind], seq=sibling)

    def out_piece(u, d):
        cols = UNIT * HEAD_SIZE
        src = ost.at[pl.ds(pl.multiple_of(peers[d] * TOKENS, TOKENS), TOKENS), pl.ds(u * cols, cols)]
        dst = out_ref.at[:, pl.ds(pl.multiple_of(head * WIDE + u * cols, cols), cols)]
        if d == 0:
            return pltpu.make_async_copy(src, dst, loc.at[4 + u])
        return remote(src, dst, out_send.at[u, d], out_recv.at[u, d], head=peers[d])

    def block_at(pos):
        pair, way = pos // 2, pos % 2
        far = (pair + 1) // 2
        other = (pair + 1) % 2 + pos // 15
        zz = (z + 8 - far + way * 2 * far) % 8
        return zz * 2 + xh + other - 2 * xh * other

    def bias_of(block):
        same = page_ref[own] == page_ref[block]
        allowed = jnp.where(same, (block < own).astype(jnp.int32), link_ref[own, block])
        return jnp.where(allowed == 1, 0.0, NEG).astype(F32)

    barrier = pltpu.get_barrier_semaphore()
    for d in range(1, 4):
        pl.semaphore_signal(barrier, inc=1, device_id={"head": peers[d]}, device_id_type=pl.DeviceIdType.MESH)
    for d in range(4):
        pl.semaphore_signal(
            barrier, inc=1, device_id={"seq": partner, "head": peers[d]}, device_id_type=pl.DeviceIdType.MESH
        )
    for to in (sibling, up, down):
        pl.semaphore_signal(barrier, inc=1, device_id={"seq": to}, device_id_type=pl.DeviceIdType.MESH)
    kv_piece(0, 0, 0).start()
    kv_piece(0, 0, 1).start()
    q_piece(0, 0).start()
    q_piece(0, 1).start()
    pl.semaphore_wait(barrier, 10)

    for kind in range(2):
        for d in range(1, 4):
            kv_piece(0, d, kind).start()
    for kind in range(2):
        for d in range(4):
            kv_piece(1, d, kind).start()
    for part in range(2):
        for d in range(1, 4):
            q_piece(d, part).start()

    def gathered(xo):
        for kind in range(2):
            for d in range(4):
                if xo == 0 and d == 0:
                    kv_piece(xo, d, kind).wait()
                else:
                    kv_piece(xo, d, kind).wait_recv()
            block = own if xo == 0 else partner // 2
            for way in range(2):
                ring(block, way, 1 + xo, kind).start()
            share(xo, block, kind).start()

    def arrived(pos):
        block, pair, way = block_at(pos), pos // 2, pos % 2

        @pl.when(pair <= 6)
        def _():
            for kind in range(2):
                ring(block, way, pair, kind).wait_recv()
                share(pos, block, kind).start()

                @pl.when(pair <= 4)
                def _():
                    ring(block, way, pair + 2, kind).start()

                @pl.when(jnp.logical_and(pair > 4, way == kind))
                def _():
                    ring(block, way, pair + 2, kind).start()

        @pl.when(pair == 7)
        def _():
            for kind in range(2):
                ring(block, kind, 7 + way, kind).wait_recv()
                share(pos, block, kind).start()

    def shared(pos, block):
        for kind in range(2):
            share(pos, block, kind).wait_recv()

    def heads(u):
        return jnp.concatenate(
            [qb[:, (u * UNIT + i) * HEAD_SIZE : (u * UNIT + i + 1) * HEAD_SIZE] for i in range(UNIT)], axis=0
        )

    def score(u, block, slot, first):
        rows = slice(u * M, (u + 1) * M)
        s = lax.dot_general(heads(u), kv[block, 0], NT, preferred_element_type=F32) * SCALE
        if first:
            token = lax.broadcasted_iota(jnp.int32, (M, BLK), 0) % ROWS + core * ROWS
            s = jnp.where(lax.broadcasted_iota(jnp.int32, (M, BLK), 1) <= token, s, NEG)
        s_s[slot] = s
        top = jnp.broadcast_to(jnp.max(s, axis=1, keepdims=True), (M, HEAD_SIZE))
        if first:
            m_s[rows] = top
            sh_s[slot] = top
        else:
            bias = bias_of(block)
            before = m_s[rows]
            after = jnp.maximum(before, top + bias)
            m_s[rows] = after
            sh_s[slot] = after - bias
            al_s[slot] = jnp.exp2(before - after)

    def weigh(u, block, slot, first):
        rows = slice(u * M, (u + 1) * M)
        shift = sh_s[slot]
        w = jnp.concatenate(
            [
                jnp.exp2(s_s[slot, :, t * HEAD_SIZE : (t + 1) * HEAD_SIZE] - shift).astype(BF16)
                for t in range(BLK // HEAD_SIZE)
            ],
            axis=1,
        )
        ones = jnp.ones((BLK, HEAD_SIZE), BF16)
        part = jnp.dot(w, jnp.concatenate([kv[block, 1], ones], axis=1), preferred_element_type=F32)
        for t in range(2):
            cols = slice(t * HEAD_SIZE, (t + 1) * HEAD_SIZE)
            acc_s[rows, cols] = part[:, cols] if first else acc_s[rows, cols] * al_s[slot] + part[:, cols]

    def finish(u):
        for i in range(UNIT):
            g = u * UNIT + i
            a = acc_s[g * ROWS : (g + 1) * ROWS, :]
            ost[:, g * HEAD_SIZE : (g + 1) * HEAD_SIZE] = (a[:, :HEAD_SIZE] / a[:, HEAD_SIZE:]).astype(BF16)

    gathered(0)
    q_piece(0, 0).wait()
    for d in range(1, 4):
        q_piece(d, 0).wait_recv()
    shared(0, own)
    other = partner // 2
    score(0, own, 0, True)
    score(1, own, 1, True)
    weigh(0, own, 0, True)
    gathered(1)
    q_piece(0, 1).wait()
    for d in range(1, 4):
        q_piece(d, 1).wait_recv()
    score(2, own, 0, True)
    weigh(1, own, 1, True)
    score(3, own, 1, True)
    weigh(2, own, 0, True)
    arrived(2)
    shared(1, other)
    score(0, other, 0, False)
    weigh(3, own, 1, True)

    def one(pos, carry):
        block, after = block_at(pos), block_at(pos + 1)
        for u in range(UNITS - 1):
            score(u + 1, block, (u + 1) % 2, False)
            weigh(u, block, u % 2, False)
            if u == 1:

                @pl.when(pos <= 13)
                def _():
                    arrived(pos + 2)

        shared(pos + 1, after)
        score(0, after, 0, False)
        weigh(UNITS - 1, block, (UNITS - 1) % 2, False)
        return carry

    lax.fori_loop(1, BLOCKS - 1, one, 0)
    last = block_at(BLOCKS - 1)
    for u in range(UNITS):
        if u < UNITS - 1:
            score(u + 1, last, (u + 1) % 2, False)
        weigh(u, last, u % 2, False)
        finish(u)
        for d in range(4):
            out_piece(u, d).start()

    for u in range(UNITS):
        out_piece(u, 0).wait()
        for d in range(1, 4):
            out_piece(u, d).wait()
    for kind in range(2):
        for d in range(1, 4):
            kv_piece(0, d, kind).wait_send()
        for d in range(4):
            kv_piece(1, d, kind).wait_send()
        for step in range(1, 7):
            for way in range(2):
                ring(own, way, step, kind).wait_send()
        for step in range(7, 9):
            ring(own, kind, step, kind).wait_send()
        for pos in range(BLOCKS):
            share(pos, own, kind).wait_send()
    for part in range(2):
        for d in range(1, 4):
            q_piece(d, part).wait_send()


def local(queries, keys, values, page_of_block, links):
    return pl.pallas_call(
        kernel,
        out_shape=jax.ShapeDtypeStruct((TOKENS, 4 * WIDE), BF16),
        in_specs=[pl.BlockSpec(memory_space=pltpu.SMEM)] * 2 + [pl.BlockSpec(memory_space=pl.ANY)] * 3,
        out_specs=pl.BlockSpec(memory_space=pl.ANY),
        scratch_shapes=[
            pltpu.VMEM((BLOCKS, 2, BLK, HEAD_SIZE), BF16),
            pltpu.VMEM((ROWS, WIDE), BF16),
            pltpu.VMEM((ROWS, WIDE), BF16),
            pltpu.VMEM((HEADS * ROWS, HEAD_SIZE), F32),
            pltpu.VMEM((HEADS * ROWS, 2 * HEAD_SIZE), F32),
            pltpu.VMEM((2, M, BLK), F32),
            pltpu.VMEM((2, M, HEAD_SIZE), F32),
            pltpu.VMEM((2, M, HEAD_SIZE), F32),
            pltpu.SemaphoreType.DMA((2, 4, 2)),
            pltpu.SemaphoreType.DMA((2, 4, 2)),
            pltpu.SemaphoreType.DMA((4, 2)),
            pltpu.SemaphoreType.DMA((4, 2)),
            pltpu.SemaphoreType.DMA((2, 9, 2)),
            pltpu.SemaphoreType.DMA((2, 9, 2)),
            pltpu.SemaphoreType.DMA((BLOCKS, 2)),
            pltpu.SemaphoreType.DMA((BLOCKS, 2)),
            pltpu.SemaphoreType.DMA((UNITS, 4)),
            pltpu.SemaphoreType.DMA((UNITS, 4)),
            pltpu.SemaphoreType.DMA((4 + UNITS,)),
        ],
        compiler_params=pltpu.CompilerParams(
            collective_id=0, has_side_effects=True, vmem_limit_bytes=60 * 2**20
        ),
    )(page_of_block, links, queries, keys, values)


def solution(mesh):
    tokens = P(("batch", "seq", "head"), None)
    in_specs = (tokens, tokens, tokens, P("batch"), P("batch", None))
    return jax.shard_map(local, mesh=mesh, in_specs=in_specs, out_specs=tokens, check_vma=False)
```

```python
import jax
import jax.numpy as jnp
from jax import lax
from jax.experimental import pallas as pl
from jax.experimental.pallas import tpu as pltpu
from jax.sharding import PartitionSpec as P

HEAD_SIZE = 128
BLK = 512
BLOCKS = 16
HEADS = 8
SEQ = 32
TOKENS = 64
ROWS = 256
WIDE = HEADS * HEAD_SIZE
UNIT = 2
UNITS = HEADS // UNIT
M = UNIT * ROWS
SCALE = HEAD_SIZE ** (-0.5) * 1.4426950408889634
NEG = -1e30
NT = (((1,), (1,)), ((), ()))
F32, BF16 = jnp.float32, jnp.bfloat16
EVENT_LEAD, TAIL = 2, 12


def kernel(
    page_ref, link_ref, q_ref, k_ref, v_ref, out_ref,
    kv, qb, ost, m_s, acc_s, s_s, sh_s, al_s, k_st, v_st, q_st,
    a2a_send, a2a_recv, q_send, q_recv, ring_send, ring_recv, sib_send, sib_recv, out_send, out_recv, loc, stage,
):
    seq, head = lax.axis_index("seq"), lax.axis_index("head")
    z, xh, core = seq // 4, (seq // 2) % 2, seq % 2
    own = seq // 2
    sibling = seq + 1 - 2 * core
    partner = seq + 2 - 4 * xh
    up, down = (seq + 4) % SEQ, (seq + SEQ - 4) % SEQ
    peers = [(head + d) % 4 for d in range(4)]
    half = pl.ds(pl.multiple_of(core * ROWS, ROWS), ROWS)

    def remote(src, dst, send, recv, **where):
        return pltpu.make_async_remote_copy(
            src_ref=src, dst_ref=dst, send_sem=send, recv_sem=recv,
            device_id=where, device_id_type=pl.DeviceIdType.MESH,
        )

    def kv_piece(xo, d, kind):
        whole = (k_ref, v_ref) if xo == 0 and d == 0 else (k_st, v_st)
        src = whole[kind].at[:, pl.ds(pl.multiple_of(peers[d] * HEAD_SIZE, HEAD_SIZE), HEAD_SIZE)]
        dst = kv.at[own, kind, pl.ds(pl.multiple_of(core * ROWS + head * TOKENS, TOKENS), TOKENS), :]
        if xo == 0 and d == 0:
            return pltpu.make_async_copy(src, dst, loc.at[kind])
        where = {"head": peers[d]} if xo == 0 else {"seq": partner, "head": peers[d]}
        return remote(src, dst, a2a_send.at[xo, d, kind], a2a_recv.at[xo, d, kind], **where)

    def q_piece(d, part):
        cols = UNIT * HEAD_SIZE
        whole = q_ref if d == 0 else q_st
        src = whole.at[:, pl.ds(pl.multiple_of(peers[d] * WIDE + part * cols, cols), cols)]
        dst = qb.at[pl.ds(pl.multiple_of(head * TOKENS, TOKENS), TOKENS), pl.ds(part * cols, cols)]
        if d == 0:
            return pltpu.make_async_copy(src, dst, loc.at[2 + part])
        return remote(src, dst, q_send.at[d, part], q_recv.at[d, part], head=peers[d])

    def ring(block, way, step, kind):
        ref = kv.at[block, kind, half, :]
        to = up + way * (down - up)
        return remote(ref, ref, ring_send.at[way, step, kind], ring_recv.at[way, step, kind], seq=to)

    def share(pos, block, kind):
        ref = kv.at[block, kind, half, :]
        return remote(ref, ref, sib_send.at[pos, kind], sib_recv.at[pos, kind], seq=sibling)

    def out_piece(u, d):
        cols = UNIT * HEAD_SIZE
        src = ost.at[pl.ds(pl.multiple_of(peers[d] * TOKENS, TOKENS), TOKENS), pl.ds(pl.multiple_of(u * cols, cols), cols)]
        dst = out_ref.at[:, pl.ds(pl.multiple_of(head * WIDE + u * cols, cols), cols)]
        if d == 0:
            return pltpu.make_async_copy(src, dst, loc.at[2 + UNITS + u])
        return remote(src, dst, out_send.at[u, d], out_recv.at[u, d], head=peers[d])

    def block_at(pos):
        pair, way = pos // 2, pos % 2
        far = (pair + 1) // 2
        other = (pair + 1) % 2 + pos // 15
        zz = (z + 8 - far + way * 2 * far) % 8
        return zz * 2 + xh + other - 2 * xh * other

    def bias_of(block):
        same = page_ref[own] == page_ref[block]
        allowed = jnp.where(same, (block < own).astype(jnp.int32), link_ref[own, block])
        return jnp.where(allowed == 1, 0.0, NEG).astype(F32)

    barrier = pltpu.get_barrier_semaphore()
    for d in range(1, 4):
        pl.semaphore_signal(barrier, inc=1, device_id={"head": peers[d]}, device_id_type=pl.DeviceIdType.MESH)
    for d in range(4):
        pl.semaphore_signal(
            barrier, inc=1, device_id={"seq": partner, "head": peers[d]}, device_id_type=pl.DeviceIdType.MESH
        )
    for to in (sibling, up, down):
        pl.semaphore_signal(barrier, inc=1, device_id={"seq": to}, device_id_type=pl.DeviceIdType.MESH)
    staged = [
        pltpu.make_async_copy(src, dst, stage.at[i])
        for i, (src, dst) in enumerate(((k_ref, k_st), (v_ref, v_st), (q_ref, q_st)))
    ]
    for copy in staged:
        copy.start()
    kv_piece(0, 0, 0).start()
    kv_piece(0, 0, 1).start()
    for part in range(UNITS):
        q_piece(0, part).start()
    pl.semaphore_wait(barrier, 10)
    staged[0].wait()
    staged[1].wait()

    for kind in range(2):
        for d in range(1, 4):
            kv_piece(0, d, kind).start()
    for kind in range(2):
        for d in range(4):
            kv_piece(1, d, kind).start()
    staged[2].wait()
    for part in range(UNITS):
        for d in range(1, 4):
            q_piece(d, part).start()

    def gathered(xo):
        for kind in range(2):
            for d in range(4):
                if xo == 0 and d == 0:
                    kv_piece(xo, d, kind).wait()
                else:
                    kv_piece(xo, d, kind).wait_recv()
            block = own if xo == 0 else partner // 2
            for way in range(2):
                ring(block, way, 1 + xo, kind).start()
            share(xo, block, kind).start()

    def arrived(event):
        pair, kind = event // 2 + 1, event % 2

        @pl.when(pair <= 6)
        def _():
            for way in range(2):
                pos = 2 * pair + way
                block = block_at(pos)
                ring(block, way, pair, kind).wait_recv()
                share(pos, block, kind).start()

                @pl.when(jnp.logical_or(pair <= 4, kind == way))
                def _():
                    ring(block, way, pair + 2, kind).start()

        @pl.when(pair == 7)
        def _():
            pos = 14 + kind
            block = block_at(pos)
            for part in range(2):
                ring(block, part, 7 + kind, part).wait_recv()
                share(pos, block, part).start()

    def shared(pos, block):
        for kind in range(2):
            share(pos, block, kind).wait_recv()

    def heads(u):
        cols = UNIT * HEAD_SIZE
        q = qb[:, u * cols : (u + 1) * cols] if isinstance(u, int) else qb[:, pl.ds(pl.multiple_of(u * cols, cols), cols)]
        return jnp.concatenate([q[:, i * HEAD_SIZE : (i + 1) * HEAD_SIZE] for i in range(UNIT)], axis=0)

    def rows_of(u):
        return slice(u * M, (u + 1) * M) if isinstance(u, int) else pl.ds(pl.multiple_of(u * M, M), M)

    def score(u, block, slot, first):
        rows = rows_of(u)
        s = lax.dot_general(heads(u), kv[block, 0], NT, preferred_element_type=F32) * SCALE
        if first:
            token = lax.broadcasted_iota(jnp.int32, (M, BLK), 0) % ROWS + core * ROWS
            s = jnp.where(lax.broadcasted_iota(jnp.int32, (M, BLK), 1) <= token, s, NEG)
        s_s[slot] = s
        top = jnp.broadcast_to(jnp.max(s, axis=1, keepdims=True), (M, HEAD_SIZE))
        if first:
            m_s[rows] = top
            sh_s[slot] = top
        else:
            bias = bias_of(block)
            before = m_s[rows]
            after = jnp.maximum(before, top + bias)
            m_s[rows] = after
            sh_s[slot] = after - bias
            al_s[slot] = jnp.exp2(before - after)

    def weigh(u, block, slot, first):
        rows = rows_of(u)
        shift = sh_s[slot]
        w = jnp.concatenate(
            [
                jnp.exp2(s_s[slot, :, t * HEAD_SIZE : (t + 1) * HEAD_SIZE] - shift).astype(BF16)
                for t in range(BLK // HEAD_SIZE)
            ],
            axis=1,
        )
        ones = jnp.ones((BLK, HEAD_SIZE), BF16)
        part = jnp.dot(w, jnp.concatenate([kv[block, 1], ones], axis=1), preferred_element_type=F32)
        for t in range(2):
            cols = slice(t * HEAD_SIZE, (t + 1) * HEAD_SIZE)
            acc_s[rows, cols] = part[:, cols] if first else acc_s[rows, cols] * al_s[slot] + part[:, cols]

    def finish(u):
        for i in range(UNIT):
            a = acc_s[pl.ds(pl.multiple_of((u * UNIT + i) * ROWS, ROWS), ROWS), :]
            cols = pl.ds(pl.multiple_of((u * UNIT + i) * HEAD_SIZE, HEAD_SIZE), HEAD_SIZE)
            ost[:, cols] = (a[:, :HEAD_SIZE] / a[:, HEAD_SIZE:]).astype(BF16)

    def queried(part):
        q_piece(0, part).wait()
        for d in range(1, 4):
            q_piece(d, part).wait_recv()

    other = partner // 2
    gathered(0)
    queried(0)
    shared(0, own)
    score(0, own, 0, True)
    weigh(0, own, 0, True)
    gathered(1)
    queried(1)
    score(1, own, 0, True)
    weigh(1, own, 0, True)
    arrived(0)
    queried(2)
    shared(1, other)
    score(0, other, 0, False)
    score(2, own, 1, True)
    weigh(0, other, 0, False)
    score(1, other, 0, False)
    weigh(2, own, 1, True)
    weigh(1, other, 0, False)
    arrived(1)
    queried(3)
    score(2, other, 0, False)
    score(3, own, 1, True)
    weigh(2, other, 0, False)
    score(3, other, 0, False)
    weigh(3, own, 1, True)
    weigh(3, other, 0, False)
    for event in range(2, 2 + EVENT_LEAD):
        arrived(event)
    shared(2, block_at(2))
    score(0, block_at(2), 0, False)

    def one(pos, carry):
        block, after = block_at(pos), block_at(pos + 1)
        arrived(pos + EVENT_LEAD)
        shared(pos + 1, after)
        for u in range(UNITS):
            if u < UNITS - 1:
                score(u + 1, block, (u + 1) % 2, False)
            else:
                score(0, after, 0, False)
            weigh(u, block, u % 2, False)
        return carry

    lax.fori_loop(2, TAIL, one, 0)
    for event in range(TAIL + EVENT_LEAD, 14):
        arrived(event)
    for pos in range(TAIL + 1, BLOCKS):
        shared(pos, block_at(pos))
    ends = [block_at(pos) for pos in range(TAIL, BLOCKS)]

    def end(u, carry):
        for i, block in enumerate(ends):
            if i < len(ends) - 1:
                score(u, ends[i + 1], (i + 1) % 2, False)
            else:
                score(jnp.minimum(u + 1, UNITS - 1), ends[0], 0, False)
            weigh(u, block, i % 2, False)
        finish(u)
        for d in range(4):
            out_piece(u, d).start()
        return carry

    lax.fori_loop(0, UNITS, end, 0)

    for u in range(UNITS):
        out_piece(u, 0).wait()
        for d in range(1, 4):
            out_piece(u, d).wait()
    for kind in range(2):
        for d in range(1, 4):
            kv_piece(0, d, kind).wait_send()
        for d in range(4):
            kv_piece(1, d, kind).wait_send()
        for step in range(1, 7):
            for way in range(2):
                ring(own, way, step, kind).wait_send()
        for step in range(7, 9):
            ring(own, kind, step, kind).wait_send()
        for pos in range(BLOCKS):
            share(pos, own, kind).wait_send()
    for part in range(UNITS):
        for d in range(1, 4):
            q_piece(d, part).wait_send()


def local(queries, keys, values, page_of_block, links):
    return pl.pallas_call(
        kernel,
        out_shape=jax.ShapeDtypeStruct((TOKENS, 4 * WIDE), BF16),
        in_specs=[pl.BlockSpec(memory_space=pltpu.SMEM)] * 2 + [pl.BlockSpec(memory_space=pl.ANY)] * 3,
        out_specs=pl.BlockSpec(memory_space=pl.ANY),
        scratch_shapes=[
            pltpu.VMEM((BLOCKS, 2, BLK, HEAD_SIZE), BF16),
            pltpu.VMEM((ROWS, WIDE), BF16),
            pltpu.VMEM((ROWS, WIDE), BF16),
            pltpu.VMEM((HEADS * ROWS, HEAD_SIZE), F32),
            pltpu.VMEM((HEADS * ROWS, 2 * HEAD_SIZE), F32),
            pltpu.VMEM((2, M, BLK), F32),
            pltpu.VMEM((2, M, HEAD_SIZE), F32),
            pltpu.VMEM((2, M, HEAD_SIZE), F32),
            pltpu.VMEM((TOKENS, 4 * HEAD_SIZE), BF16),
            pltpu.VMEM((TOKENS, 4 * HEAD_SIZE), BF16),
            pltpu.VMEM((TOKENS, 4 * WIDE), BF16),
            pltpu.SemaphoreType.DMA((2, 4, 2)),
            pltpu.SemaphoreType.DMA((2, 4, 2)),
            pltpu.SemaphoreType.DMA((4, UNITS)),
            pltpu.SemaphoreType.DMA((4, UNITS)),
            pltpu.SemaphoreType.DMA((2, 9, 2)),
            pltpu.SemaphoreType.DMA((2, 9, 2)),
            pltpu.SemaphoreType.DMA((BLOCKS, 2)),
            pltpu.SemaphoreType.DMA((BLOCKS, 2)),
            pltpu.SemaphoreType.DMA((UNITS, 4)),
            pltpu.SemaphoreType.DMA((UNITS, 4)),
            pltpu.SemaphoreType.DMA((2 + 2 * UNITS,)),
            pltpu.SemaphoreType.DMA((3,)),
        ],
        compiler_params=pltpu.CompilerParams(
            collective_id=0, has_side_effects=True, vmem_limit_bytes=60 * 2**20
        ),
    )(page_of_block, links, queries, keys, values)


def solution(mesh):
    tokens = P(("batch", "seq", "head"), None)
    in_specs = (tokens, tokens, tokens, P("batch"), P("batch", None))
    return jax.shard_map(local, mesh=mesh, in_specs=in_specs, out_specs=tokens, check_vma=False)
```
